32 devices in a mesh: var: 8 (over z, core), samp: 4 (over y, x).
Axes of the slice: x: 2, y: 2, z: 4, core: 2. Of those that a mesh axis runs over, the one named last changes fastest.
Arguments:
- geno: bfloat16 [8192, 16384], P('samp', 'var'), may hold values from -5 to 5
- scale_index: int32 [64, 16384], P('samp', 'var'), may hold values from 0 to 15
- scale_table: float32 [16], replicated, may hold values from 0.25 to 4
- residual: float32 [8, 8192], P(None, 'samp'), may hold values from -6 to 6
- beta_active: float32 [8, 3584], P(None, 'var'), may hold values from -6 to 6
- block_inverse: float32 [16, 256, 256], P('var'), may hold values from -1 to 4
- active_ids: int32 [3584], P('var'), may hold values from 0 to 16383, as said below
- admit_ids: int32 [512], P('var'), may hold values from 0 to 16383, as said below
Outputs:
- scores: float32 [8, 16384], P(None, 'var')
- coefficients: float32 [8, 4096], P(None, 'var')
- residual_out: float32 [8, 8192], P(None, 'samp')
The draws below stay inside these ranges and needn't reach their ends.
Inputs may be any that keep to these rules, and one draw needn't show every extreme that they name: Variant ids, all different from one another and from those of admit_ids. The fitting slots of one index of var are its 448 entries of active_ids followed by its 64 entries of admit_ids; of these 512 slots at most 128 name variants held by any one index of var, and for every index of var some one holder reaches exactly 128. `admit_ids`: variant ids, as for active_ids.
All inputs are finite; a program needn't handle non-finite values.
Results may differ from the reference program's by a relative error of at most 0.004.
Values may be sent and summed in bfloat16 or wider, within the bound.
A program may use at most 128 MiB of HBM per device.

```python
import math
import jax
import jax.numpy as jnp
from jax import lax

PHENO = 8
BLOCK = 256
GROUP = 128
LEVELS = 16
PASSES = 3
VAR_DEV = 2048
ADM_DEV = 64
FIT_DEV = 512
ACT_DEV = 448
SAMPLES = 8192
VARIANTS = 16384
ACTIVE = 3584
FIT = 4096
NBLK = 16
N_VAR = 8


def fit_layout(key):
    base_key = jax.random.fold_in(key, 7)
    holders = N_VAR
    capacity = 2 * FIT_DEV // holders
    pairing = jax.vmap(lambda keyed: jax.random.permutation(keyed, holders))(jax.random.split(jax.random.fold_in(base_key, 1), holders))
    shares = jax.random.randint(jax.random.fold_in(base_key, 2), (holders, holders // 2), 0, capacity + 1, dtype=jnp.int32)
    shares = shares.at[:, 0].set(0)
    paired = jnp.stack([capacity - shares, shares], -1).reshape(holders, holders)
    rows_index = jnp.arange(holders, dtype=jnp.int32)[:, None]
    counts = jnp.zeros((holders, holders), jnp.int32).at[rows_index, pairing].set(paired)
    finish = jnp.cumsum(counts, 1)
    anchor = finish - counts
    slot_range = jnp.arange(FIT_DEV, dtype=jnp.int32)
    holder = jnp.sum((finish[:, None, :] <= slot_range[None, :, None]).astype(jnp.int32), -1)
    serial = slot_range[None, :] - jnp.take_along_axis(anchor, holder, 1)
    offsets = jnp.cumsum(counts, 0) - counts
    shuffled = jax.vmap(lambda keyed: jax.random.permutation(keyed, VAR_DEV))(jax.random.split(jax.random.fold_in(base_key, 3), holders))
    column = shuffled[holder, jnp.take_along_axis(offsets, holder, 1) + serial]
    chosen = holder * VAR_DEV + column
    reorder = jax.vmap(lambda keyed: jax.random.permutation(keyed, FIT_DEV))(jax.random.split(jax.random.fold_in(base_key, 4), holders))
    return jnp.take_along_axis(chosen, reorder, 1).astype(jnp.int32)


def draw_active_ids(key, part):
    return fit_layout(key)[:, :ACT_DEV].reshape(-1)


def draw_admit_ids(key, part):
    return fit_layout(key)[:, ACT_DEV:].reshape(-1)


def draw_block_inverse(key, part):
    noise = jax.random.normal(jax.random.fold_in(key, 11), (NBLK, BLOCK, BLOCK), jnp.float32)
    diagonal = jnp.exp(jax.random.uniform(jax.random.fold_in(key, 12), (NBLK, BLOCK), jnp.float32, 0.0, 0.6931))
    spread = 0.35
    symmetric = (noise + jnp.swapaxes(noise, 1, 2)) * (spread / (2.0 * BLOCK) ** 0.5)
    return jnp.eye(BLOCK, dtype=jnp.float32)[None, :, :] * diagonal[:, :, None] + symmetric


def set_ends(drawn, key, smallest, largest):
    longest = drawn.shape.index(max(drawn.shape))
    spots = []
    for shift in (0, 1):
        where = [jax.random.randint(jax.random.fold_in(key, axis), (), 0, length) for axis, length in enumerate(drawn.shape)]
        where[longest] = (where[longest] + shift) % drawn.shape[longest]
        spots.append(tuple(where))
    return drawn.at[spots[0]].set(smallest).at[spots[1]].set(largest)


def block_scale(own_key, extent, pieces, low, top_value):
    loudness, own = 1.0, jax.random.fold_in(own_key, 6)
    for dim, blocks in pieces:
        steps = jnp.exp(jax.random.uniform(jax.random.fold_in(own, dim), (blocks,), jnp.float32, low / len(pieces), top_value / len(pieces)))
        loudness = loudness * jnp.repeat(steps, extent[dim] // blocks).reshape([-1 if axis == dim else 1 for axis in range(len(extent))])
    return loudness


def gaussian(rng, extent, width, bound, shards=(), kind=jnp.bfloat16):
    entries = jax.random.normal(rng, extent, jnp.float32) * width
    if len(shards) > 0:
        entries = block_scale(rng, extent, shards, -0.22, 0.18) * entries
    return jnp.clip(entries, min=-bound, max=bound).astype(kind)


def setup_inputs(seed: int = 0) -> dict:
    key_of = jax.random.split(jax.random.key(seed), 9)
    geno = gaussian(key_of[0], (SAMPLES, VARIANTS), 1.0, 5.0, ((0, 4), (1, 8)))
    scale_index = set_ends(jax.random.randint(key_of[1], (SAMPLES // GROUP, VARIANTS), 0, LEVELS), jax.random.fold_in(key_of[1], 1), 0, LEVELS - 1).astype(jnp.int32)
    scale_table = jnp.clip(jnp.exp(jax.random.uniform(key_of[2], (LEVELS,), jnp.float32, math.log(0.25), math.log(4.0))), 0.25, 4.0)
    residual = gaussian(key_of[3], (PHENO, SAMPLES), 1.0, 6.0, ((1, 4),), jnp.float32)
    beta_active = gaussian(key_of[4], (PHENO, ACTIVE), 1.0, 6.0, ((1, 8),), jnp.float32)
    block_inverse = draw_block_inverse(jax.random.fold_in(key_of[8], 71), 0)
    active_ids = draw_active_ids(jax.random.fold_in(key_of[8], 71), 0)
    admit_ids = draw_admit_ids(jax.random.fold_in(key_of[8], 71), 0)
    return {"geno": geno, "scale_index": scale_index, "scale_table": scale_table, "residual": residual, "beta_active": beta_active, "block_inverse": block_inverse, "active_ids": active_ids, "admit_ids": admit_ids}


penalty = 0.5
epsilon = 1e-06

def dequantize(values, indices, lookup):
    groups = indices.shape[0]
    scales = lookup[indices]
    widened = values.reshape(groups, values.shape[0] // groups, values.shape[1]).astype(jnp.float32) * scales[:, None, :]
    return widened.reshape(values.shape).astype(jnp.bfloat16)

def reference(geno, scale_index, scale_table, residual, beta_active, block_inverse, active_ids, admit_ids):
    inv_root = 1.0 / math.sqrt(SAMPLES)
    resid_low = residual.astype(jnp.bfloat16)

    def screen_block(block_index):
        first_column = block_index * VAR_DEV
        values = lax.dynamic_slice_in_dim(geno, first_column, VAR_DEV, 1)
        indices = lax.dynamic_slice_in_dim(scale_index, first_column, VAR_DEV, 1)
        return jnp.dot(resid_low, dequantize(values, indices, scale_table), preferred_element_type=jnp.float32)
    blocks = lax.map(screen_block, jnp.arange(N_VAR, dtype=jnp.int32))
    scores = jnp.transpose(blocks, (1, 0, 2)).reshape(PHENO, VARIANTS) * inv_root
    fit_ids = jnp.concatenate([active_ids.reshape(N_VAR, ACT_DEV), admit_ids.reshape(N_VAR, ADM_DEV)], 1).reshape(FIT)
    fitting = dequantize(jnp.take(geno, fit_ids, axis=1), jnp.take(scale_index, fit_ids, axis=1), scale_table)
    coeffs = jnp.concatenate([beta_active.reshape(PHENO, N_VAR, ACT_DEV), jnp.zeros((PHENO, N_VAR, ADM_DEV), jnp.float32)], 2).reshape(PHENO, FIT)
    current = residual
    for pass_index in range(PASSES):
        gradient = jnp.dot(current.astype(jnp.bfloat16), fitting, preferred_element_type=jnp.float32) * inv_root
        inner_term = (gradient - penalty * coeffs).reshape(PHENO, NBLK, BLOCK)
        direction = jnp.einsum('bij,pbj->pbi', block_inverse, inner_term, precision=lax.Precision.HIGHEST)
        direction = direction.reshape(PHENO, FIT).astype(jnp.bfloat16)
        update = jnp.dot(direction, fitting.T, preferred_element_type=jnp.float32) * inv_root
        cross_sum = lax.optimization_barrier(jnp.sum(current * update, 1))
        square = lax.optimization_barrier(jnp.sum(update * update, 1)) + epsilon
        factor = (cross_sum / square)[:, None]
        current = current - factor * update
        coeffs = coeffs + factor * direction.astype(jnp.float32)
    return (scores, coeffs, current)
```

```python
import functools
import math

import jax
import jax.numpy as jnp
from jax import lax
from jax.experimental import pallas as pl
from jax.experimental.pallas import tpu as pltpu
from jax.sharding import PartitionSpec as P

PASSES = 3
PENALTY = 0.5
EPSILON = 1e-06
LANES = 128
F32 = jnp.float32
BF16 = jnp.bfloat16
NN = (((1,), (0,)), ((), ()))
NT = (((1,), (1,)), ((), ()))


def dot(a, b, dims=NN):
    return lax.dot_general(a, b, dims, preferred_element_type=F32)


def split(x):
    high = x.astype(BF16).astype(F32)
    return jnp.concatenate([high, x - high], axis=0).astype(BF16)


def joined(x):
    half = x.shape[0] // 2
    return x[:half] + x[half:]


def kernel(
    V, S, pad,
    geno, sidx, table, resid, beta, binv, ids_in,
    scores_out, coef_out, resid_out,
    x_ref, scale_ref, rlow, part, pick, unpick, tri, inv_hi, inv_lo, ids_all, src_row,
    packed, d_got, d_held, up_two, coef, grad, direct, own_up,
    send_a, recv_a, send_b, recv_b, send_c, recv_c, recv_u, recv_p, send_s, recv_s,
    load_sem, send_sem, recv_sem,
):
    N = V * S
    rows, width = x_ref.shape
    groups = sidx.shape[0]
    per_group = rows // groups
    levels = table.shape[0]
    ph = resid.shape[0]
    fit = ids_in.shape[1]
    blocks, bsize = binv.shape[0], binv.shape[1]
    chunk = rows // V
    step = 2 * per_group
    n_steps = rows // step
    inv_root = 1.0 / math.sqrt(rows * S)
    mv, ms = lax.axis_index("var"), lax.axis_index("samp")
    me = ms * V + mv

    def load(i):
        at = pl.ds(pl.multiple_of(i * step, step), step)
        return pltpu.make_async_copy(geno.at[at], x_ref.at[at], load_sem.at[i])

    for i in range(n_steps):
        load(i).start()

    barrier = pltpu.get_barrier_semaphore()

    def other(k):
        t = lax.rem(me + k, N)
        return lax.div(t, V), lax.rem(t, V)

    def greet(k, c):
        s, v = other(k)
        pl.semaphore_signal(
            barrier, inc=1, device_id={"var": v, "samp": s}, device_id_type=pl.DeviceIdType.MESH
        )
        return c

    lax.fori_loop(1, N, greet, 0)

    def send(src, dst, sem, v, s):
        pltpu.make_async_remote_copy(
            src_ref=src, dst_ref=dst, send_sem=send_sem.at[sem], recv_sem=recv_sem.at[sem],
            device_id={"var": v, "samp": s}, device_id_type=pl.DeviceIdType.MESH,
        ).start()

    def got(ref, sem):
        pltpu.make_async_copy(ref, ref, recv_sem.at[sem]).wait()

    def sent(ref, sem):
        pltpu.make_async_copy(ref, ref, send_sem.at[sem]).wait()

    def var_peers(fn):
        def one(k, c):
            fn(lax.rem(mv + k, V))
            return c

        lax.fori_loop(1, V, one, 0)

    IDS, A, B, C, U, SC, SM = 0, 1, 1 + PASSES, 1 + 2 * PASSES, 1 + 3 * PASSES, 1 + 4 * PASSES, 2 + 4 * PASSES

    ids_all[mv] = ids_in[...]
    index = sidx[...]
    scales = jnp.zeros(index.shape, F32)
    for level in range(levels):
        scales = jnp.where(index == level, table[level], scales)
    scale_ref[...] = scales
    rlow[...] = resid[...].astype(BF16)
    for b in range(blocks):
        whole = binv[b]
        high = whole.astype(BF16)
        inv_hi[b] = high
        inv_lo[b] = (whole - high.astype(F32)).astype(BF16)
    kept = beta.shape[1]
    coef[...] = jnp.zeros((ph, fit), F32)
    coef[:, 0:kept] = beta[...]
    tri[...] = jnp.where(
        lax.broadcasted_iota(jnp.int32, (fit, fit), 0) < lax.broadcasted_iota(jnp.int32, (fit, fit), 1),
        1.0, 0.0,
    ).astype(BF16)

    pl.semaphore_wait(barrier, N - 1)
    var_peers(lambda v: send(ids_all.at[mv], ids_all.at[mv], IDS, v, ms))

    part[...] = jnp.zeros((ph, width), F32)
    cols = 512

    def screen(i, c):
        load(i).wait()
        for half in range(2):
            at = pl.ds(pl.multiple_of(i * step + half * per_group, per_group), per_group)
            for j in range(width // cols):
                lane = slice(j * cols, (j + 1) * cols)
                scale = scale_ref[pl.ds(2 * i + half, 1), lane]
                x_ref[at, lane] = (x_ref[at, lane].astype(F32) * scale).astype(BF16)
        at = pl.ds(pl.multiple_of(i * step, step), step)
        part[...] += dot(rlow[:, at], x_ref[at, :])
        return c

    lax.fori_loop(0, n_steps, screen, 0)
    recv_p[ms] = part[...]

    got(ids_all.at[pl.ds(0, V - 1)], IDS)
    line = lax.broadcasted_iota(jnp.int32, (V, fit), 0)
    all_ids = jnp.zeros((V, fit), jnp.int32)
    for g in range(V):
        all_ids = jnp.where(line == g, ids_all[g][0:1], all_ids)
    column = all_ids - mv * width
    held = (column >= 0) & (column < width)
    serial = dot(jnp.where(held, 1.0, 0.0).astype(BF16), tri[...]).astype(jnp.int32)
    serial = jnp.where(held, serial, -1)
    column = jnp.where(held, column, 0)
    eight = lax.broadcasted_iota(jnp.int32, (8, fit), 0)
    turn = lax.broadcasted_iota(jnp.int32, (pad, fit), 0)
    for g in range(V):
        col = column[g:g + 1]
        digits = jnp.where(
            eight == 0, lax.shift_right_logical(col, 7),
            jnp.where(eight == 1, col & 127, jnp.where(eight == 2, 1, 0)),
        ).astype(F32).astype(BF16)
        place = jnp.where(turn == serial[g:g + 1], 1.0, 0.0).astype(BF16)
        found = dot(digits, place, NT)
        where = jnp.where(found[2:3] > 0.5, found[0:1] * 128.0 + found[1:2], -1.0)
        src_row[g] = jnp.broadcast_to(where.astype(jnp.int32), (8, pad))

    def mark(i, c):
        at = pl.ds(pl.multiple_of(i * 256, 256), 256)
        here = lax.broadcasted_iota(jnp.int32, (256, pad), 0) + i * 256
        for g in range(V):
            pick[at, g * pad:(g + 1) * pad] = jnp.where(here == src_row[g][0:1], 1.0, 0.0).astype(BF16)
        return c

    lax.fori_loop(0, width // 256, mark, 0)

    mine = ids_in[0:1] - line * width
    marks = jnp.where((mine >= 0) & (mine < width), 1.0, 0.0)
    before = dot(marks.astype(BF16), tri[...])
    position = jnp.sum(marks * (before + line.astype(F32) * float(pad)), axis=0, keepdims=True)
    position = position.astype(jnp.int32)

    def place_own(i, c):
        at = pl.ds(pl.multiple_of(i * 128, 128), 128)
        here = lax.broadcasted_iota(jnp.int32, (128, fit), 0) + i * 128
        unpick[at, :] = jnp.where(here == position, 1.0, 0.0).astype(BF16)
        return c

    lax.fori_loop(0, V * pad // 128, place_own, 0)

    resid_out[...] = resid[...]
    lane = lax.broadcasted_iota(jnp.int32, (ph, LANES), 1)

    def length(total):
        return total[:, 0:1] / (total[:, 1:2] + EPSILON)

    def step_sums(p):
        cur = resid_out[:, pl.ds(pl.multiple_of(mv * chunk, chunk), chunk)]
        upd = own_up[...]
        cross = jnp.sum(cur * upd, axis=1, keepdims=True)
        square = jnp.sum(upd * upd, axis=1, keepdims=True)
        return jnp.where(lane == 0, cross, jnp.where(lane == 1, square, 0.0))

    def advance(factor, p):
        for v in range(V):
            at = slice(v * chunk, (v + 1) * chunk)
            resid_out[:, at] = resid_out[:, at] - factor * recv_u[p, v]

    sums = jnp.zeros((ph, LANES), F32)
    for p in range(PASSES):
        up_two[...] = split(part[...])
        wide = 2 * pad

        for n in range(V * pad // wide):
            out = joined(dot(up_two[...], pick[:, n * wide:(n + 1) * wide]))
            for q in range(2):
                send_a[p, 2 * n + q, 0:ph] = out[:, q * pad:(q + 1) * pad]
                send_a[p, 2 * n + q, ph:2 * ph] = jnp.broadcast_to(sums, (ph, LANES))

        def route(k, c):
            s, v = other(k)
            send(send_a.at[p, v], recv_a.at[p, me], A + p, v, s)
            return c

        lax.fori_loop(1, N, route, 0)
        recv_a[p, me] = send_a[p, mv]
        if p == 0:
            def share(k, c):
                send(recv_p.at[ms], recv_p.at[ms], SC, mv, lax.rem(ms + k, S))
                return c

            lax.fori_loop(1, S, share, 0)
        got(recv_a.at[p, pl.ds(0, N - 1)], A + p)
        for v in range(V):
            val = recv_a[p, v, 0:ph]
            for s in range(1, S):
                val = val + recv_a[p, s * V + v, 0:ph]
            packed[:, v * pad:(v + 1) * pad] = split(val)
        slots = joined(dot(packed[...], unpick[...])) * inv_root
        if p == 0:
            grad[...] = slots
        else:
            total = recv_a[p, 0, ph:2 * ph]
            for n in range(1, N):
                total = total + recv_a[p, n, ph:2 * ph]
            factor = length(total)
            grad[...] = grad[...] - factor * slots
            coef[...] = coef[...] + factor * direct[...].astype(F32)
        inner = grad[...] - PENALTY * coef[...]
        for b in range(blocks):
            at = slice(b * bsize, (b + 1) * bsize)
            two = split(inner[:, at])
            main = joined(dot(two, inv_hi[b], NT))
            rest = dot(two, inv_lo[b], NT)
            direct[:, at] = (main + rest[:ph]).astype(BF16)

        back = dot(direct[...], unpick[...], NT)
        for v in range(V):
            send_b[p, v] = back[:, v * pad:(v + 1) * pad]
        var_peers(lambda v: send(send_b.at[p, v], recv_b.at[p, mv], B + p, v, ms))
        recv_b[p, mv] = send_b[p, mv]
        if p > 0:
            advance(factor, p - 1)
        got(recv_b.at[p, pl.ds(0, V - 1)], B + p)
        for v in range(V):
            d_got[:, v * pad:(v + 1) * pad] = recv_b[p, v].astype(BF16)
        def spread(i, c):
            at = pl.ds(pl.multiple_of(i * 512, 512), 512)
            d_held[:, at] = dot(d_got[...], pick[at, :], NT).astype(BF16)
            return c

        lax.fori_loop(0, width // 512, spread, 0)

        def piece(v):
            at = pl.ds(pl.multiple_of(v * chunk, chunk), chunk)
            return dot(d_held[...], x_ref[at, :], NT)

        def give(v):
            send_c[p, v] = piece(v)
            send(send_c.at[p, v], recv_c.at[p, mv], C + p, v, ms)

        var_peers(give)
        recv_c[p, mv] = piece(mv)
        got(recv_c.at[p, pl.ds(0, V - 1)], C + p)
        val = recv_c[p, 0]
        for v in range(1, V):
            val = val + recv_c[p, v]
        val = val * inv_root
        own_up[...] = val
        recv_u[p, mv] = val
        sums = step_sums(p)
        if p + 1 == PASSES:
            send_s[...] = sums
            recv_s[me] = sums

            def tell(k, c):
                s, v = other(k)
                send(send_s, recv_s.at[me], SM, v, s)
                return c

            var_peers(lambda v: send(recv_u.at[p, mv], recv_u.at[p, mv], U + p, v, ms))
            lax.fori_loop(1, N, tell, 0)
        else:
            var_peers(lambda v: send(recv_u.at[p, mv], recv_u.at[p, mv], U + p, v, ms))
        got(recv_u.at[p, pl.ds(0, V - 1)], U + p)
        if p + 1 < PASSES:
            for v in range(V):
                up_two[:, v * chunk:(v + 1) * chunk] = split(recv_u[p, v])

            def project(i, c):
                at = pl.ds(pl.multiple_of(i * 256, 256), 256)
                part[:, at] = joined(dot(up_two[...], x_ref[:, at]))
                return c

            lax.fori_loop(0, width // 256, project, 0)

    got(recv_p.at[pl.ds(0, S - 1)], SC)
    val = recv_p[0]
    for s in range(1, S):
        val = val + recv_p[s]
    scores_out[...] = val * inv_root
    got(recv_s.at[pl.ds(0, N - 1)], SM)
    total = recv_s[0]
    for n in range(1, N):
        total = total + recv_s[n]
    factor = length(total)
    advance(factor, PASSES - 1)
    coef_out[...] = coef[...] + factor * direct[...].astype(F32)

    sent(ids_all.at[pl.ds(0, V - 1)], IDS)
    sent(recv_p.at[pl.ds(0, S - 1)], SC)
    sent(recv_s.at[pl.ds(0, N - 1)], SM)
    for p in range(PASSES):
        sent(recv_a.at[p, pl.ds(0, N - 1)], A + p)
        sent(recv_b.at[p, pl.ds(0, V - 1)], B + p)
        sent(recv_c.at[p, pl.ds(0, V - 1)], C + p)
        sent(recv_u.at[p, pl.ds(0, V - 1)], U + p)


def on_device(geno, scale_index, scale_table, residual, beta_active, block_inverse, active_ids, admit_ids):
    V, S = lax.axis_size("var"), lax.axis_size("samp")
    N = V * S
    rows, width = geno.shape
    ph = residual.shape[0]
    ids = jnp.concatenate([active_ids, admit_ids])
    fit = ids.shape[0]
    pad = LANES * pl.cdiv(2 * fit // V, LANES)
    ids = jnp.broadcast_to(ids[None, :], (8, fit))
    chunk = rows // V
    vmem = pl.BlockSpec(memory_space=pltpu.VMEM)
    n_sem = 3 + 4 * PASSES
    return pl.pallas_call(
        functools.partial(kernel, V, S, pad),
        out_shape=(
            jax.ShapeDtypeStruct((ph, width), F32),
            jax.ShapeDtypeStruct((ph, fit), F32),
            jax.ShapeDtypeStruct((ph, rows), F32),
        ),
        in_specs=[
            pl.BlockSpec(memory_space=pl.ANY), vmem, pl.BlockSpec(memory_space=pltpu.SMEM),
            vmem, vmem, vmem, vmem,
        ],
        out_specs=(vmem, vmem, vmem),
        scratch_shapes=[
            pltpu.VMEM((rows, width), BF16),
            pltpu.VMEM(scale_index.shape, F32),
            pltpu.VMEM((ph, rows), BF16),
            pltpu.VMEM((ph, width), F32),
            pltpu.VMEM((width, V * pad), BF16),
            pltpu.VMEM((V * pad, fit), BF16),
            pltpu.VMEM((fit, fit), BF16),
            pltpu.VMEM(block_inverse.shape, BF16),
            pltpu.VMEM(block_inverse.shape, BF16),
            pltpu.VMEM((V, 8, fit), jnp.int32),
            pltpu.VMEM((V, 8, pad), jnp.int32),
            pltpu.VMEM((2 * ph, V * pad), BF16),
            pltpu.VMEM((ph, V * pad), BF16),
            pltpu.VMEM((ph, width), BF16),
            pltpu.VMEM((2 * ph, width), BF16),
            pltpu.VMEM((ph, fit), F32),
            pltpu.VMEM((ph, fit), F32),
            pltpu.VMEM((ph, fit), BF16),
            pltpu.VMEM((ph, chunk), F32),
            pltpu.VMEM((PASSES, V, 2 * ph, pad), F32),
            pltpu.VMEM((PASSES, N, 2 * ph, pad), F32),
            pltpu.VMEM((PASSES, V, ph, pad), F32),
            pltpu.VMEM((PASSES, V, ph, pad), F32),
            pltpu.VMEM((PASSES, V, ph, chunk), F32),
            pltpu.VMEM((PASSES, V, ph, chunk), F32),
            pltpu.VMEM((PASSES, V, ph, chunk), F32),
            pltpu.VMEM((S, ph, width), F32),
            pltpu.VMEM((ph, LANES), F32),
            pltpu.VMEM((N, ph, LANES), F32),
            pltpu.SemaphoreType.DMA((rows // (2 * (rows // scale_index.shape[0])),)),
            pltpu.SemaphoreType.DMA((n_sem,)),
            pltpu.SemaphoreType.DMA((n_sem,)),
        ],
        compiler_params=pltpu.CompilerParams(
            collective_id=0, has_side_effects=True, vmem_limit_bytes=60 * 1024 * 1024
        ),
    )(geno, scale_index, scale_table, residual, beta_active, block_inverse, ids)


def solution(mesh):
    placed = (
        P("samp", "var"), P("samp", "var"), P(), P(None, "samp"), P(None, "var"),
        P("var", None, None), P("var"), P("var"),
    )
    return jax.shard_map(
        on_device, mesh=mesh, in_specs=placed,
        out_specs=(P(None, "var"), P(None, "var"), P(None, "samp")), check_vma=False,
    )
```

```python
import functools
import math

import jax
import jax.numpy as jnp
from jax import lax
from jax.experimental import pallas as pl
from jax.experimental.pallas import tpu as pltpu
from jax.sharding import PartitionSpec as P

PASSES = 3
PENALTY = 0.5
EPSILON = 1e-06
LANES = 128
F32 = jnp.float32
BF16 = jnp.bfloat16
NN = (((1,), (0,)), ((), ()))
NT = (((1,), (1,)), ((), ()))


def dot(a, b, dims=NN):
    return lax.dot_general(a, b, dims, preferred_element_type=F32)


def split(x):
    high = x.astype(BF16).astype(F32)
    return jnp.concatenate([high, x - high], axis=0).astype(BF16)


def joined(x):
    half = x.shape[0] // 2
    return x[:half] + x[half:]


def kernel(
    V, S, pad,
    geno, sidx, table, resid, beta, binv, active, admit,
    scores_out, coef_out, resid_out,
    x_ref, scale_ref, rlow, part, pick, unpick, tri, inv_hi, inv_lo, ids_all, src_row,
    packed, d_got, d_held, up_two, coef, grad, direct,
    send_a, recv_a, send_b, recv_b, send_c, recv_c, recv_u, recv_p, recv_s,
    load_sem, send_sem, recv_sem,
):
    N = V * S
    rows, width = x_ref.shape
    groups = sidx.shape[0]
    per_group = rows // groups
    levels = table.shape[0]
    ph = resid.shape[0]
    kept = active.shape[1]
    fit = kept + admit.shape[1]
    blocks, bsize = binv.shape[0], binv.shape[1]
    chunk = rows // V
    step = 2 * per_group
    n_steps = rows // step
    inv_root = 1.0 / math.sqrt(rows * S)
    mv, ms = lax.axis_index("var"), lax.axis_index("samp")
    me = ms * V + mv

    def load(i):
        at = pl.ds(pl.multiple_of(i * step, step), step)
        return pltpu.make_async_copy(geno.at[at], x_ref.at[at], load_sem.at[i])

    for i in range(n_steps):
        load(i).start()

    barrier = pltpu.get_barrier_semaphore()

    def other(k):
        t = lax.rem(me + k, N)
        return lax.div(t, V), lax.rem(t, V)

    def greet(k, c):
        s, v = other(k)
        pl.semaphore_signal(
            barrier, inc=1, device_id={"var": v, "samp": s}, device_id_type=pl.DeviceIdType.MESH
        )
        return c

    lax.fori_loop(1, N, greet, 0)

    def send(src, dst, sem, v, s):
        pltpu.make_async_remote_copy(
            src_ref=src, dst_ref=dst, send_sem=send_sem.at[sem], recv_sem=recv_sem.at[sem],
            device_id={"var": v, "samp": s}, device_id_type=pl.DeviceIdType.MESH,
        ).start()

    def got(ref, sem):
        pltpu.make_async_copy(ref, ref, recv_sem.at[sem]).wait()

    def sent(ref, sem):
        pltpu.make_async_copy(ref, ref, send_sem.at[sem]).wait()

    def var_peers(fn):
        def one(k, c):
            fn(lax.rem(mv + k, V))
            return c

        lax.fori_loop(1, V, one, 0)

    IDS, A, B, C, U, SC, SM = 0, 1, 1 + PASSES, 1 + 2 * PASSES, 1 + 3 * PASSES, 1 + 4 * PASSES, 2 + 4 * PASSES

    ids_all[mv, :, 0:kept] = jnp.broadcast_to(active[...], (8, kept))
    ids_all[mv, :, kept:fit] = jnp.broadcast_to(admit[...], (8, fit - kept))
    index = sidx[...]
    scales = jnp.zeros(index.shape, F32)
    for level in range(levels):
        scales = jnp.where(index == level, table[level], scales)
    scale_ref[...] = scales
    rlow[...] = resid[...].astype(BF16)
    for b in range(blocks):
        whole = binv[b]
        high = whole.astype(BF16)
        inv_hi[b] = high
        inv_lo[b] = (whole - high.astype(F32)).astype(BF16)
    coef[...] = jnp.zeros((ph, fit), F32)
    coef[:, 0:kept] = beta[...]
    tri[...] = jnp.where(
        lax.broadcasted_iota(jnp.int32, (fit, fit), 0) < lax.broadcasted_iota(jnp.int32, (fit, fit), 1),
        1.0, 0.0,
    ).astype(BF16)

    pl.semaphore_wait(barrier, N - 1)
    var_peers(lambda v: send(ids_all.at[mv], ids_all.at[mv], IDS, v, ms))

    part[...] = jnp.zeros((ph, width), F32)
    cols = 512

    def screen(i, c):
        load(i).wait()
        for half in range(2):
            at = pl.ds(pl.multiple_of(i * step + half * per_group, per_group), per_group)
            for j in range(width // cols):
                lane = slice(j * cols, (j + 1) * cols)
                scale = scale_ref[pl.ds(2 * i + half, 1), lane]
                x_ref[at, lane] = (x_ref[at, lane].astype(F32) * scale).astype(BF16)
        at = pl.ds(pl.multiple_of(i * step, step), step)
        part[...] += dot(rlow[:, at], x_ref[at, :])
        return c

    lax.fori_loop(0, n_steps, screen, 0)
    recv_p[ms] = part[...]

    got(ids_all.at[pl.ds(0, V - 1)], IDS)
    line = lax.broadcasted_iota(jnp.int32, (V, fit), 0)
    all_ids = jnp.zeros((V, fit), jnp.int32)
    for g in range(V):
        all_ids = jnp.where(line == g, ids_all[g][0:1], all_ids)
    column = all_ids - mv * width
    held = (column >= 0) & (column < width)
    serial = dot(jnp.where(held, 1.0, 0.0).astype(BF16), tri[...]).astype(jnp.int32)
    serial = jnp.where(held, serial, -1)
    column = jnp.where(held, column, 0)
    eight = lax.broadcasted_iota(jnp.int32, (8, fit), 0)
    turn = lax.broadcasted_iota(jnp.int32, (pad, fit), 0)
    for g in range(V):
        col = column[g:g + 1]
        digits = jnp.where(
            eight == 0, lax.shift_right_logical(col, 7),
            jnp.where(eight == 1, col & 127, jnp.where(eight == 2, 1, 0)),
        ).astype(F32).astype(BF16)
        place = jnp.where(turn == serial[g:g + 1], 1.0, 0.0).astype(BF16)
        found = dot(digits, place, NT)
        where = jnp.where(found[2:3] > 0.5, found[0:1] * 128.0 + found[1:2], -1.0)
        src_row[g] = jnp.broadcast_to(where.astype(jnp.int32), (8, pad))

    def mark(i, c):
        at = pl.ds(pl.multiple_of(i * 256, 256), 256)
        here = lax.broadcasted_iota(jnp.int32, (256, pad), 0) + i * 256
        for g in range(V):
            pick[at, g * pad:(g + 1) * pad] = jnp.where(here == src_row[g][0:1], 1.0, 0.0).astype(BF16)
        return c

    lax.fori_loop(0, width // 256, mark, 0)

    mine = ids_all[mv][0:1] - line * width
    marks = jnp.where((mine >= 0) & (mine < width), 1.0, 0.0)
    before = dot(marks.astype(BF16), tri[...])
    position = jnp.sum(marks * (before + line.astype(F32) * float(pad)), axis=0, keepdims=True)
    position = position.astype(jnp.int32)

    def place_own(i, c):
        at = pl.ds(pl.multiple_of(i * 128, 128), 128)
        here = lax.broadcasted_iota(jnp.int32, (128, fit), 0) + i * 128
        unpick[at, :] = jnp.where(here == position, 1.0, 0.0).astype(BF16)
        return c

    lax.fori_loop(0, V * pad // 128, place_own, 0)

    resid_out[...] = resid[...]
    lane = lax.broadcasted_iota(jnp.int32, (ph, LANES), 1)

    def length(p):
        got(recv_s.at[p, pl.ds(0, S - 1)], SM + p)
        total = recv_s[p, 0]
        for s in range(1, S):
            total = total + recv_s[p, s]
        return total[:, 0:1] / (total[:, 1:2] + EPSILON)

    def tell_sums(p):
        cross = jnp.zeros((ph, chunk), F32)
        square = jnp.zeros((ph, chunk), F32)
        for v in range(V):
            upd = recv_u[p, v]
            cross = cross + resid_out[:, v * chunk:(v + 1) * chunk] * upd
            square = square + upd * upd
        cross = jnp.sum(cross, axis=1, keepdims=True)
        square = jnp.sum(square, axis=1, keepdims=True)
        recv_s[p, ms] = jnp.where(lane == 0, cross, jnp.where(lane == 1, square, 0.0))

        def tell(k, c):
            send(recv_s.at[p, ms], recv_s.at[p, ms], SM + p, mv, lax.rem(ms + k, S))
            return c

        lax.fori_loop(1, S, tell, 0)

    def advance(factor, p):
        for v in range(V):
            at = slice(v * chunk, (v + 1) * chunk)
            resid_out[:, at] = resid_out[:, at] - factor * recv_u[p, v]

    for p in range(PASSES):
        up_two[...] = split(part[...])
        wide = 2 * pad

        for n in range(V * pad // wide):
            out = joined(dot(up_two[...], pick[:, n * wide:(n + 1) * wide]))
            for q in range(2):
                send_a[p, 2 * n + q] = out[:, q * pad:(q + 1) * pad].astype(BF16)

        def route(k, c):
            s, v = other(k)
            send(send_a.at[p, v], recv_a.at[p, me], A + p, v, s)
            return c

        lax.fori_loop(1, N, route, 0)
        recv_a[p, me] = send_a[p, mv]
        if p == 0:
            def share(k, c):
                send(recv_p.at[ms], recv_p.at[ms], SC, mv, lax.rem(ms + k, S))
                return c

            lax.fori_loop(1, S, share, 0)
        got(recv_a.at[p, pl.ds(0, N - 1)], A + p)
        for v in range(V):
            val = recv_a[p, v].astype(F32)
            for s in range(1, S):
                val = val + recv_a[p, s * V + v].astype(F32)
            packed[:, v * pad:(v + 1) * pad] = split(val)
        slots = joined(dot(packed[...], unpick[...])) * inv_root
        if p == 0:
            grad[...] = slots
        else:
            factor = length(p - 1)
            grad[...] = grad[...] - factor * slots
            coef[...] = coef[...] + factor * direct[...].astype(F32)
        inner = grad[...] - PENALTY * coef[...]
        for b in range(blocks):
            at = slice(b * bsize, (b + 1) * bsize)
            two = split(inner[:, at])
            main = joined(dot(two, inv_hi[b], NT))
            rest = dot(two, inv_lo[b], NT)
            direct[:, at] = (main + rest[:ph]).astype(BF16)

        back = dot(direct[...], unpick[...], NT)
        for v in range(V):
            send_b[p, v] = back[:, v * pad:(v + 1) * pad].astype(BF16)
        var_peers(lambda v: send(send_b.at[p, v], recv_b.at[p, mv], B + p, v, ms))
        recv_b[p, mv] = send_b[p, mv]
        if p > 0:
            advance(factor, p - 1)
        got(recv_b.at[p, pl.ds(0, V - 1)], B + p)
        for v in range(V):
            d_got[:, v * pad:(v + 1) * pad] = recv_b[p, v]
        def spread(i, c):
            at = pl.ds(pl.multiple_of(i * 512, 512), 512)
            d_held[:, at] = dot(d_got[...], pick[at, :], NT).astype(BF16)
            return c

        lax.fori_loop(0, width // 512, spread, 0)

        def piece(v):
            at = pl.ds(pl.multiple_of(v * chunk, chunk), chunk)
            return dot(d_held[...], x_ref[at, :], NT)

        def give(v):
            send_c[p, v] = piece(v).astype(BF16)
            send(send_c.at[p, v], recv_c.at[p, mv], C + p, v, ms)

        var_peers(give)
        recv_c[p, mv] = piece(mv).astype(BF16)
        got(recv_c.at[p, pl.ds(0, V - 1)], C + p)
        val = recv_c[p, 0].astype(F32)
        for v in range(1, V):
            val = val + recv_c[p, v].astype(F32)
        val = val * inv_root
        recv_u[p, mv] = val
        var_peers(lambda v: send(recv_u.at[p, mv], recv_u.at[p, mv], U + p, v, ms))
        got(recv_u.at[p, pl.ds(0, V - 1)], U + p)
        tell_sums(p)
        if p + 1 < PASSES:
            for v in range(V):
                up_two[:, v * chunk:(v + 1) * chunk] = split(recv_u[p, v])

            def project(i, c):
                at = pl.ds(pl.multiple_of(i * 256, 256), 256)
                part[:, at] = joined(dot(up_two[...], x_ref[:, at]))
                return c

            lax.fori_loop(0, width // 256, project, 0)

    got(recv_p.at[pl.ds(0, S - 1)], SC)
    val = recv_p[0]
    for s in range(1, S):
        val = val + recv_p[s]
    scores_out[...] = val * inv_root
    factor = length(PASSES - 1)
    advance(factor, PASSES - 1)
    coef_out[...] = coef[...] + factor * direct[...].astype(F32)

    sent(ids_all.at[pl.ds(0, V - 1)], IDS)
    sent(recv_p.at[pl.ds(0, S - 1)], SC)
    for p in range(PASSES):
        sent(recv_a.at[p, pl.ds(0, N - 1)], A + p)
        sent(recv_s.at[p, pl.ds(0, S - 1)], SM + p)
        sent(recv_b.at[p, pl.ds(0, V - 1)], B + p)
        sent(recv_c.at[p, pl.ds(0, V - 1)], C + p)
        sent(recv_u.at[p, pl.ds(0, V - 1)], U + p)


def on_device(geno, scale_index, scale_table, residual, beta_active, block_inverse, active_ids, admit_ids):
    V, S = lax.axis_size("var"), lax.axis_size("samp")
    N = V * S
    rows, width = geno.shape
    ph = residual.shape[0]
    fit = active_ids.shape[0] + admit_ids.shape[0]
    pad = LANES * pl.cdiv(2 * fit // V, LANES)
    chunk = rows // V
    vmem = pl.BlockSpec(memory_space=pltpu.VMEM)
    n_sem = 2 + 5 * PASSES
    return pl.pallas_call(
        functools.partial(kernel, V, S, pad),
        out_shape=(
            jax.ShapeDtypeStruct((ph, width), F32),
            jax.ShapeDtypeStruct((ph, fit), F32),
            jax.ShapeDtypeStruct((ph, rows), F32),
        ),
        in_specs=[
            pl.BlockSpec(memory_space=pl.ANY), vmem, pl.BlockSpec(memory_space=pltpu.SMEM),
            vmem, vmem, vmem, vmem, vmem,
        ],
        out_specs=(vmem, vmem, vmem),
        scratch_shapes=[
            pltpu.VMEM((rows, width), BF16),
            pltpu.VMEM(scale_index.shape, F32),
            pltpu.VMEM((ph, rows), BF16),
            pltpu.VMEM((ph, width), F32),
            pltpu.VMEM((width, V * pad), BF16),
            pltpu.VMEM((V * pad, fit), BF16),
            pltpu.VMEM((fit, fit), BF16),
            pltpu.VMEM(block_inverse.shape, BF16),
            pltpu.VMEM(block_inverse.shape, BF16),
            pltpu.VMEM((V, 8, fit), jnp.int32),
            pltpu.VMEM((V, 8, pad), jnp.int32),
            pltpu.VMEM((2 * ph, V * pad), BF16),
            pltpu.VMEM((ph, V * pad), BF16),
            pltpu.VMEM((ph, width), BF16),
            pltpu.VMEM((2 * ph, width), BF16),
            pltpu.VMEM((ph, fit), F32),
            pltpu.VMEM((ph, fit), F32),
            pltpu.VMEM((ph, fit), BF16),
            pltpu.VMEM((PASSES, V, ph, pad), BF16),
            pltpu.VMEM((PASSES, N, ph, pad), BF16),
            pltpu.VMEM((PASSES, V, ph, pad), BF16),
            pltpu.VMEM((PASSES, V, ph, pad), BF16),
            pltpu.VMEM((PASSES, V, ph, chunk), BF16),
            pltpu.VMEM((PASSES, V, ph, chunk), BF16),
            pltpu.VMEM((PASSES, V, ph, chunk), F32),
            pltpu.VMEM((S, ph, width), F32),
            pltpu.VMEM((PASSES, S, ph, LANES), F32),
            pltpu.SemaphoreType.DMA((rows // (2 * (rows // scale_index.shape[0])),)),
            pltpu.SemaphoreType.DMA((n_sem,)),
            pltpu.SemaphoreType.DMA((n_sem,)),
        ],
        compiler_params=pltpu.CompilerParams(
            collective_id=0, has_side_effects=True, vmem_limit_bytes=60 * 1024 * 1024
        ),
    )(geno, scale_index, scale_table, residual, beta_active, block_inverse, active_ids[None], admit_ids[None])


def solution(mesh):
    placed = (
        P("samp", "var"), P("samp", "var"), P(), P(None, "samp"), P(None, "var"),
        P("var", None, None), P("var"), P("var"),
    )
    return jax.shard_map(
        on_device, mesh=mesh, in_specs=placed,
        out_specs=(P(None, "var"), P(None, "var"), P(None, "samp")), check_vma=False,
    )
```
